32 devices in a mesh: groups: 2 (over y), wide: 8 (over z, x), narrow: 2 (over core).
Axes of the slice: x: 2, y: 2, z: 4, core: 2. Of those that a mesh axis runs over, the one named last changes fastest.
Arguments:
- queries: bfloat16 [4, 2048, 64], P(('groups', 'narrow'), 'wide'), parts along dimension 0, may hold values from -6 to 6
- key_rows: bfloat16 [4, 2048, 64], P(('groups', 'narrow'), 'wide'), parts along dimension 0, may hold values from -6 to 6
- values: bfloat16 [4, 2048, 64], P(('groups', 'narrow'), 'wide'), parts along dimension 0, may hold values from -6 to 6
- log_gate: float32 [4, 2048], P(('groups', 'narrow'), 'wide'), parts along dimension 0, may hold values from -0.8 to 0, as said below
- lengths: int32 [4], P(('groups', 'narrow')), parts along dimension 0, may hold values from 1024 to 2048
- cont_queries: bfloat16 [160, 64], P(('groups', 'wide', 'narrow')), parts along dimension 0, may hold values from -6 to 6
- cont_prompt: int32 [160], P(('groups', 'wide', 'narrow')), parts along dimension 0, may hold values from 0 to 1
Outputs:
- prompt_out: bfloat16 [4, 2048, 64], P(('groups', 'narrow'), 'wide'), parts along dimension 0
- cont_out: bfloat16 [160, 64], P(('groups', 'wide', 'narrow')), parts along dimension 0
The draws below stay inside these ranges and needn't reach their ends.
There are 2 independent parts, one for each index of `groups`. The reference program is written for one: setup_inputs(seed, part) draws one part's arguments, and reference() takes and returns one part's arrays. A program takes and returns all parts, laid end to end along the dimension named above; each array names one. Nothing has to cross between parts.
Inputs may be any that keep to these rules, and one draw needn't show every extreme that they name: `log_gate`: gates only shrink the state: every entry is at most zero.
All inputs are finite; a program needn't handle non-finite values.
Results may differ from the reference program's by a relative error of at most 0.0067.
Values may be sent and summed in bfloat16 or wider, within the bound.
No kernel may reach another device: no remote copies, remote signals or barrier semaphores. Data moves between devices by JAX's collectives and lax.ppermute only.
A program may use at most 64 MiB of HBM per device.

```python
import jax
import jax.numpy as jnp
from jax import lax

D = 64
TOK = 256
PROMPTS = 2
SEQ = 2048
CONT = 80
N_WIDE = 8


def draw_log_gate(key, part):
    streams = jax.random.split(jax.random.fold_in(key, 11), 6)
    slow_rate = jax.random.uniform(streams[0], (PROMPTS,), jnp.float32, 0.2, 0.6) / SEQ
    fast_rate = 1.0 / jnp.exp(jax.random.uniform(streams[1], (PROMPTS,), jnp.float32, jnp.log(30.0), jnp.log(50.0)))
    chosen = jax.random.randint(streams[2], (), 0, PROMPTS)
    forget_speed = jnp.where(jnp.arange(PROMPTS) == chosen, fast_rate, slow_rate)
    forget_multiplier = jnp.exp(jax.random.uniform(streams[3], (PROMPTS, SEQ), jnp.float32, jnp.log(0.5), jnp.log(2.0)))
    spots = jax.random.randint(streams[4], (PROMPTS, 2), 0, SEQ)
    deviation_sums = jax.random.uniform(streams[5], (PROMPTS, 2), jnp.float32, 0.2, 0.5)
    agreeing_number = jnp.arange(SEQ)[None, :, None] == spots[:, None, :]
    span_extent = jnp.sum(jnp.where(agreeing_number, jnp.log(1.0 - deviation_sums)[:, None, :], 0.0), axis=2)
    return (-forget_speed[:, None] * forget_multiplier + span_extent).astype(jnp.float32)


def touch_ends(entries, rng, low, top_value):
    shape = entries.shape
    place = [jax.random.randint(jax.random.fold_in(rng, axis), (), 0, shape[axis]) for axis in range(len(shape))]
    entries = entries.at[tuple(place)].set(low)
    longest = shape.index(max(shape))
    place[longest] = (place[longest] + 1) % shape[longest]
    return entries.at[tuple(place)].set(top_value)


def block_levels(stream_key, extent, shards, least, largest):
    level, own = 1.0, jax.random.fold_in(stream_key, 6)
    for dim, parts in shards:
        steps = jnp.exp(jax.random.uniform(jax.random.fold_in(own, dim), (parts,), jnp.float32, least / len(shards), largest / len(shards)))
        level = level * jnp.repeat(steps, extent[dim] // parts).reshape([-1 if axis == dim else 1 for axis in range(len(extent))])
    return level


def gaussian(stream_key, shape, scale, limit, cuts=(), held_as=jnp.bfloat16):
    entries = scale * jax.random.normal(stream_key, shape, jnp.float32)
    if cuts:
        entries = entries * block_levels(stream_key, shape, cuts, -0.22, 0.18)
    return jnp.clip(entries, -limit, limit).astype(held_as)


def setup_inputs(seed: int = 0, part: int = 0) -> dict:
    key_list = jax.random.split(jax.random.key(seed), 8)
    part_splits = jax.random.split(jax.random.fold_in(key_list[7], part), 8)
    return {
        "queries": gaussian(part_splits[0], (PROMPTS, SEQ, D), 1.0, 6.0, ((0, 2), (1, 8))),
        "key_rows": gaussian(part_splits[1], (PROMPTS, SEQ, D), 1.0, 6.0, ((0, 2), (1, 8))),
        "values": gaussian(part_splits[2], (PROMPTS, SEQ, D), 1.0, 6.0, ((0, 2), (1, 8))),
        "log_gate": draw_log_gate(jax.random.fold_in(jax.random.fold_in(key_list[7], part), 71), part),
        "lengths": jax.random.randint(part_splits[4], (PROMPTS,), SEQ // 2, SEQ + 1).astype(jnp.int32),
        "cont_queries": gaussian(part_splits[5], (CONT, D), 1.0, 6.0, ((0, 16),)),
        "cont_prompt": touch_ends(jax.random.randint(part_splits[6], (CONT,), 0, PROMPTS), jax.random.fold_in(part_splits[6], 1), 0, PROMPTS - 1).astype(jnp.int32),
    }


epsilon = 1e-06

def rms_rows(running):
    return running * lax.rsqrt(lax.optimization_barrier(jnp.mean(running * running, axis=-1, keepdims=True)) + epsilon)

def pair_features(rows):
    wide_rows = rows.astype(jnp.float32)
    outer = wide_rows[:, :, None] * wide_rows[:, None, :]
    return outer.reshape(rows.shape[0], rows.shape[1] * rows.shape[1]).astype(jnp.bfloat16)

def shard_pass(query_rows, key_rows, payload_lines, gate_log, live_mask, carried):
    row_count, head_width = key_rows.shape
    gate_live = gate_log * live_mask
    cumulative = jnp.cumsum(gate_live)
    scores = lax.dot_general(query_rows, key_rows, (((1,), (1,)), ((), ())), preferred_element_type=jnp.float32)
    row_ids = jnp.arange(row_count, dtype=jnp.int32)
    lower_mask = row_ids[:, None] >= row_ids[None, :]
    decay_matrix = jnp.exp(jnp.where(lower_mask, cumulative[:, None] - cumulative[None, :], -jnp.inf))
    weights = (scores * scores * decay_matrix * live_mask[None, :]).astype(jnp.bfloat16)
    local_term = jnp.dot(weights, payload_lines, preferred_element_type=jnp.float32)
    carried_term = jnp.dot(pair_features(query_rows), carried, preferred_element_type=jnp.float32)
    running = local_term + jnp.exp(cumulative)[:, None] * carried_term
    output = (live_mask[:, None] * rms_rows(running)).astype(jnp.bfloat16)
    piece_number = cumulative[-1]
    scaled = live_mask * jnp.exp(piece_number - cumulative)
    spread = (scaled[:, None] * payload_lines.astype(jnp.float32)).astype(jnp.bfloat16)
    span_state = lax.dot_general(pair_features(key_rows), spread, (((0,), (0,)), ((), ())), preferred_element_type=jnp.float32)
    return (output, span_state.astype(jnp.bfloat16), piece_number)

def prompt_pass(query_everything, key_all, value_all, gate_all, length):
    position = jnp.arange(SEQ, dtype=jnp.int32)
    live_all = (position < length).astype(jnp.float32)

    def shard_step(carry, shard_item):
        query_rows, key_rows, payload_lines, gate_log, live_mask = shard_item
        output, span_state, piece_number = shard_pass(query_rows, key_rows, payload_lines, gate_log, live_mask, carry.astype(jnp.bfloat16))
        carry = jnp.exp(piece_number) * carry + span_state.astype(jnp.float32)
        return (carry, output)
    shard_items = (query_everything.reshape(N_WIDE, TOK, D), key_all.reshape(N_WIDE, TOK, D), value_all.reshape(N_WIDE, TOK, D), gate_all.reshape(N_WIDE, TOK), live_all.reshape(N_WIDE, TOK))
    initial = jnp.zeros((D * D, D), jnp.float32)
    final_state, outputs = lax.scan(shard_step, initial, shard_items)
    return (outputs.reshape(SEQ, D), final_state.astype(jnp.bfloat16))

def reference(queries, key_rows, values, log_gate, lengths, cont_queries, cont_prompt):
    outputs = []
    running = jnp.zeros((CONT, D), jnp.float32)
    cont_pairs = pair_features(cont_queries)
    for prompt_index in range(PROMPTS):
        output, final_state = prompt_pass(queries[prompt_index], key_rows[prompt_index], values[prompt_index], log_gate[prompt_index], lengths[prompt_index])
        outputs.append(output)
        partial_value = jnp.dot(cont_pairs, final_state, preferred_element_type=jnp.float32)
        running = jnp.where((cont_prompt == prompt_index)[:, None], partial_value, running)
    return (jnp.stack(outputs), rms_rows(running).astype(jnp.bfloat16))
```

```python
import jax
import jax.numpy as jnp
import numpy as np
from jax import lax
from jax.experimental import pallas as pl
from jax.experimental.pallas import tpu as pltpu
from jax.sharding import PartitionSpec as P

epsilon = 1e-06
block_rows = 1024
extra_rows = 16


def rms_rows(running):
    return running * lax.rsqrt(jnp.mean(running * running, axis=-1, keepdims=True) + epsilon)


def extend_zeros(table, pad_count):
    return np.concatenate([table, np.zeros((pad_count,), table.dtype)])


def pair_tables(head_width, shard_count):
    lead_index, trail_index = np.triu_indices(head_width)
    doubled = np.where(lead_index == trail_index, 1.0, 2.0)
    feature_count = lead_index.shape[0]
    padded_rows = -(-feature_count // shard_count) * shard_count
    block_width = min(block_rows, padded_rows)
    full_length = -(-padded_rows // block_width) * block_width
    pad_count = full_length - lead_index.shape[0]
    lead_index = extend_zeros(lead_index, pad_count).astype(np.int32)
    trail_index = extend_zeros(trail_index, pad_count).astype(np.int32)
    doubled = extend_zeros(doubled, pad_count).astype(np.float32)
    live_pairs = (doubled > 0).astype(np.float32)
    return (
        jnp.asarray(lead_index),
        jnp.asarray(trail_index),
        jnp.asarray(doubled),
        jnp.asarray(live_pairs),
        padded_rows,
        block_width,
        full_length,
    )


def pair_block(rows, lead_part, trail_part, forget_multiplier):
    leading_columns = jnp.take(rows, lead_part, axis=1).astype(jnp.float32)
    right_cols = jnp.take(rows, trail_part, axis=1).astype(jnp.float32)
    return (leading_columns * right_cols * forget_multiplier[None, :]).astype(jnp.bfloat16)


def block_state(key_rows, spread, tables):
    lead_all, trail_all, doubled_all, live_pairs, padded_rows, block_width, full_length = tables
    head_width = key_rows.shape[1]

    def fill_block(block_index, state):
        first_row = block_index * block_width
        features = pair_block(
            key_rows,
            lax.dynamic_slice_in_dim(lead_all, first_row, block_width),
            lax.dynamic_slice_in_dim(trail_all, first_row, block_width),
            lax.dynamic_slice_in_dim(live_pairs, first_row, block_width),
        )
        state_block = lax.dot_general(
            features, spread, (((0,), (0,)), ((), ())), preferred_element_type=jnp.float32
        )
        return lax.dynamic_update_slice_in_dim(
            state, state_block.astype(jnp.bfloat16), first_row, 0
        )

    initial = jnp.zeros((full_length, head_width), jnp.bfloat16)
    return lax.fori_loop(0, full_length // block_width, fill_block, initial)[:padded_rows]


def carried_read(query_rows, carried, tables):
    lead_all, trail_all, doubled_all, live_pairs, padded_rows, block_width, full_length = tables
    row_count, head_width = query_rows.shape
    if full_length > padded_rows:
        carried = jnp.pad(carried, ((0, full_length - padded_rows), (0, 0)))

    def add_block(block_index, running):
        first_row = block_index * block_width
        features = pair_block(
            query_rows,
            lax.dynamic_slice_in_dim(lead_all, first_row, block_width),
            lax.dynamic_slice_in_dim(trail_all, first_row, block_width),
            lax.dynamic_slice_in_dim(doubled_all, first_row, block_width),
        )
        state_rows = lax.dynamic_slice_in_dim(carried, first_row, block_width, 0)
        return running + jnp.dot(features, state_rows, preferred_element_type=jnp.float32)

    return lax.fori_loop(
        0, full_length // block_width, add_block, jnp.zeros((row_count, head_width), jnp.float32)
    )


def owner_prefix(sent_slices, totals):
    shard_count = totals.shape[0]
    inclusive = jnp.cumsum(totals)
    exclusive = jnp.concatenate([jnp.zeros((1,), jnp.float32), inclusive])
    target = lax.iota(jnp.int32, shard_count + 1)[:, None]
    source = lax.iota(jnp.int32, shard_count)[None, :]
    weight = jnp.exp(jnp.where(source < target, exclusive[:, None] - inclusive[None, :], -jnp.inf))
    return jnp.einsum(
        "wu,urn->wrn", weight, sent_slices.astype(jnp.float32), precision=lax.Precision.HIGHEST
    )


def prompt_rows(query_rows, key_rows, payload_lines, cumulative, live_mask, carried, tables):
    row_count, head_width = query_rows.shape
    scores = lax.dot_general(
        query_rows, key_rows, (((1,), (1,)), ((), ())), preferred_element_type=jnp.float32
    )
    row_ids = lax.iota(jnp.int32, row_count)
    lower_mask = row_ids[:, None] >= row_ids[None, :]
    decay_matrix = jnp.exp(
        jnp.where(lower_mask, cumulative[:, None] - cumulative[None, :], -jnp.inf)
    )
    weights = (scores * scores * decay_matrix * live_mask[None, :]).astype(jnp.bfloat16)
    local_term = jnp.dot(weights, payload_lines, preferred_element_type=jnp.float32)
    carried_term = carried_read(query_rows, carried, tables)
    running = local_term + jnp.exp(cumulative)[:, None] * carried_term
    return (live_mask[:, None] * rms_rows(running)).astype(jnp.bfloat16)


def on_device(queries, key_rows, values, log_gate, lengths, cont_queries, cont_prompt):
    wide_count = lax.axis_size("wide")
    lane_count = lax.axis_size("narrow")
    owner_index = lax.axis_index("wide")
    prompt_lane = lax.axis_index("narrow")
    query_rows = queries[0]
    own_keys = key_rows[0]
    payload_lines = values[0]
    row_count, head_width = own_keys.shape
    tables = pair_tables(head_width, wide_count)
    lead_all, trail_all, doubled_all = (tables[0], tables[1], tables[2])
    padded_rows = tables[4]
    rows_per = padded_rows // wide_count
    position = owner_index * row_count + lax.iota(jnp.int32, row_count)
    live_mask = (position < lengths[0]).astype(jnp.float32)
    cumulative = jnp.cumsum(log_gate[0] * live_mask)
    piece_number = cumulative[-1]
    scaled = live_mask * jnp.exp(piece_number - cumulative)
    spread = (scaled[:, None] * payload_lines.astype(jnp.float32)).astype(jnp.bfloat16)
    span_state = block_state(own_keys, spread, tables)
    totals = lax.all_gather(piece_number[None], "wide", axis=0, tiled=True)
    sent_slices = lax.all_to_all(
        span_state.reshape(wide_count, rows_per, head_width),
        "wide",
        split_axis=0,
        concat_axis=0,
        tiled=True,
    )
    rounded = owner_prefix(sent_slices, totals).astype(jnp.bfloat16)
    carried_slices = lax.all_to_all(
        rounded[:wide_count], "wide", split_axis=0, concat_axis=0, tiled=True
    )
    carried = carried_slices.reshape(padded_rows, head_width)
    final_slice = rounded[wide_count]
    prompt_out = prompt_rows(
        query_rows, own_keys, payload_lines, cumulative, live_mask, carried, tables
    )
    prompt_ids = lax.iota(jnp.int32, lane_count)[:, None]
    chosen = (cont_prompt[None, :] == prompt_ids)[:, :, None]
    masked = jnp.where(chosen, cont_queries[None, :, :], jnp.zeros_like(cont_queries)[None, :, :])
    pair_rows = lax.all_gather(masked, "narrow", axis=1, tiled=True)
    own_rows = lax.dynamic_index_in_dim(pair_rows, prompt_lane, 0, keepdims=False)
    initial = jnp.zeros((own_rows.shape[0], head_width), jnp.float32)
    shard_portion = lax.all_gather(final_slice, "wide", axis=0, tiled=True)
    piece_rows = shard_portion.shape[0]
    features = pair_block(
        own_rows,
        lax.slice_in_dim(lead_all, 0, piece_rows, axis=0),
        lax.slice_in_dim(trail_all, 0, piece_rows, axis=0),
        lax.slice_in_dim(doubled_all, 0, piece_rows, axis=0),
    )
    partial_value = initial + jnp.dot(features, shard_portion, preferred_element_type=jnp.float32)
    running = lax.psum_scatter(partial_value, "narrow", scatter_dimension=0, tiled=True)
    cont_out = rms_rows(running).astype(jnp.bfloat16)
    return (prompt_out[None], cont_out)


def split_three(x):
    first = x.astype(jnp.bfloat16)
    rest = x - first.astype(jnp.float32)
    second = rest.astype(jnp.bfloat16)
    third = (rest - second.astype(jnp.float32)).astype(jnp.bfloat16)
    return first, second, third


def gate_row(gate_ref, length, owner_index):
    row_count = gate_ref.shape[1]
    position = owner_index * row_count + lax.broadcasted_iota(jnp.int32, (1, row_count), 1)
    live = (position < length).astype(jnp.float32)
    return gate_ref[...] * live, live


def live_column(length, owner_index, row_count):
    position = owner_index * row_count + lax.broadcasted_iota(jnp.int32, (row_count, 1), 0)
    return (position < length).astype(jnp.float32)


def square_ids(row_count):
    shape = (row_count, row_count)
    return lax.broadcasted_iota(jnp.int32, shape, 0), lax.broadcasted_iota(jnp.int32, shape, 1)


def pack_kernel(length_ref, gate_ref, key_ref, value_ref, out_ref):
    row_count, head_width = key_ref.shape
    owner_index = lax.axis_index("wide")
    length = length_ref[0]
    gates, _ = gate_row(gate_ref, length, owner_index)
    row_ids, col_ids = square_ids(row_count)
    later = jnp.sum(jnp.where(col_ids > row_ids, gates, 0.0), axis=1, keepdims=True)
    total = jnp.sum(gates, axis=1, keepdims=True)
    scaled = live_column(length, owner_index, row_count) * jnp.exp(later)
    spread = (scaled * value_ref[...].astype(jnp.float32)).astype(jnp.bfloat16)
    out_ref[:row_count, :] = jnp.concatenate([key_ref[...], spread], axis=1)
    first, second, third = split_three(total)
    tail = lax.broadcasted_iota(jnp.int32, (extra_rows, 2 * head_width), 0)
    parts = jnp.where(
        tail == 0,
        first.astype(jnp.float32),
        jnp.where(
            tail == 1,
            second.astype(jnp.float32),
            jnp.where(tail == 2, third.astype(jnp.float32), 0.0),
        ),
    )
    out_ref[row_count:, :] = parts.astype(jnp.bfloat16)


def block_total(message_ref, row_count):
    tail = message_ref[row_count:, :].astype(jnp.float32)
    return tail[0:1, 0:1] + tail[1:2, 0:1] + tail[2:3, 0:1]


def squared_read(query_rows, message_ref, row_count, head_width):
    keys = message_ref[:row_count, :head_width]
    spread = message_ref[:row_count, head_width:]
    scores = lax.dot_general(
        query_rows, keys, (((1,), (1,)), ((), ())), preferred_element_type=jnp.float32
    )
    weights = (scores * scores).astype(jnp.bfloat16)
    return jnp.dot(weights, spread, preferred_element_type=jnp.float32)


def between(totals, owners, after, before):
    picked = jnp.zeros((1, 1), jnp.float32)
    for total, owner in zip(totals, owners):
        inside = jnp.logical_and(owner > after, owner < before)
        picked = picked + jnp.where(inside, total, 0.0)
    return picked


def near_kernel(
    length_ref, gate_ref, query_ref, key_ref, value_ref, cont_ref, *refs
):
    messages, (half_ref, reach_ref) = refs[:-2], refs[-2:]
    row_count, head_width = key_ref.shape
    owner_index = lax.axis_index("wide")
    length = length_ref[0]
    gates, live = gate_row(gate_ref, length, owner_index)
    row_ids, col_ids = square_ids(row_count)
    upper = (row_ids <= col_ids).astype(jnp.bfloat16)
    cumulative_row = jnp.zeros((1, row_count), jnp.float32)
    for part in split_three(jnp.broadcast_to(gates, (8, row_count))):
        cumulative_row = cumulative_row + jnp.dot(
            part, upper, preferred_element_type=jnp.float32
        )[:1]
    cumulative = jnp.sum(jnp.where(col_ids <= row_ids, gates, 0.0), axis=1, keepdims=True)
    query_rows = query_ref[...]
    scores = lax.dot_general(
        query_rows, key_ref[...], (((1,), (1,)), ((), ())), preferred_element_type=jnp.float32
    )
    decay = jnp.exp(jnp.where(col_ids <= row_ids, cumulative - cumulative_row, -jnp.inf))
    weights = (scores * scores * decay * live).astype(jnp.bfloat16)
    total = jnp.dot(weights, value_ref[...], preferred_element_type=jnp.float32)
    owners = [owner_index ^ step for step in range(len(messages))]
    totals = [block_total(m, row_count) for m in messages]
    half_end = (owner_index | (len(messages) - 1)) + 1
    carried = jnp.zeros((row_count, head_width), jnp.float32)
    reach = jnp.zeros(reach_ref.shape, jnp.float32)
    cont_rows = cont_ref[...]
    for step, message in enumerate(messages):
        if step:
            scale = jnp.exp(between(totals, owners, owners[step], owner_index))
            scale = jnp.where(owners[step] < owner_index, scale, 0.0)
            carried = carried + scale * squared_read(query_rows, message, row_count, head_width)
        rest = jnp.exp(between(totals, owners, owners[step], half_end))
        reach = reach + rest * squared_read(cont_rows, message, row_count, head_width)
    half_ref[...] = total + jnp.exp(cumulative) * carried
    reach_ref[...] = reach


def far_parts(own_refs, far_refs, row_count):
    count = len(own_refs)
    owner_index = lax.axis_index("wide")
    owners = [owner_index ^ step for step in range(count)]
    far_owners = [owner_index ^ (step + count) for step in range(count)]
    totals = [block_total(m, row_count) for m in own_refs]
    far_totals = [block_total(m, row_count) for m in far_refs]
    return owner_index, owners, far_owners, totals, far_totals


def reach_kernel(cont_ref, reach_ref, *refs):
    out_ref = refs[-1]
    count = (len(refs) - 1) // 2
    own_refs, far_refs = refs[:count], refs[count:-1]
    head_width = cont_ref.shape[1]
    row_count = own_refs[0].shape[0] - extra_rows
    owner_index, owners, far_owners, totals, far_totals = far_parts(own_refs, far_refs, row_count)
    far_end = (far_owners[0] | (count - 1)) + 1
    far_reach = jnp.zeros(out_ref.shape, jnp.float32)
    for owner, message in zip(far_owners, far_refs):
        scale = jnp.exp(between(far_totals, far_owners, owner, far_end))
        far_reach = far_reach + scale * squared_read(
            cont_ref[...], message, row_count, head_width
        )
    is_upper = far_owners[0] < owner_index
    own_scale = jnp.where(is_upper, 1.0, jnp.exp(sum(far_totals)))
    far_scale = jnp.where(is_upper, jnp.exp(sum(totals)), 1.0)
    out_ref[...] = own_scale * reach_ref[...] + far_scale * far_reach


def far_kernel(length_ref, gate_ref, query_ref, half_ref, *refs):
    out_ref = refs[-1]
    count = (len(refs) - 1) // 2
    own_refs, far_refs = refs[:count], refs[count:-1]
    row_count, head_width = query_ref.shape
    owner_index, owners, far_owners, totals, far_totals = far_parts(own_refs, far_refs, row_count)
    length = length_ref[0]
    gates, _ = gate_row(gate_ref, length, owner_index)
    row_ids, col_ids = square_ids(row_count)
    cumulative = jnp.sum(jnp.where(col_ids <= row_ids, gates, 0.0), axis=1, keepdims=True)
    before = between(totals, owners, -1, owner_index)
    far_end = (far_owners[0] | (count - 1)) + 1
    carried = jnp.zeros((row_count, head_width), jnp.float32)
    for owner, message in zip(far_owners, far_refs):
        scale = jnp.exp(between(far_totals, far_owners, owner, far_end) + before)
        scale = jnp.where(owner < owner_index, scale, 0.0)
        carried = carried + scale * squared_read(query_ref[...], message, row_count, head_width)
    total = half_ref[...] + jnp.exp(cumulative) * carried
    normed = rms_rows(total)
    out_ref[...] = (live_column(length, owner_index, row_count) * normed).astype(jnp.bfloat16)


def call_kernel(body, operands, shapes, flops):
    specs = [
        pl.BlockSpec(memory_space=pltpu.SMEM)
        if operand.ndim == 1
        else pl.BlockSpec(memory_space=pltpu.VMEM)
        for operand in operands
    ]
    outs = [pl.BlockSpec(memory_space=pltpu.VMEM) for _ in shapes]
    single = len(shapes) == 1
    return pl.pallas_call(
        body,
        out_shape=shapes[0] if single else shapes,
        in_specs=specs,
        out_specs=outs[0] if single else outs,
        cost_estimate=pl.CostEstimate(flops=flops, bytes_accessed=flops // 64, transcendentals=0),
    )(*operands)


def gathered_device(queries, key_rows, values, log_gate, lengths, cont_queries, cont_prompt):
    wide_count = lax.axis_size("wide")
    half = wide_count // 2
    lane = lax.axis_index("narrow")
    query_rows, own_keys, payload_lines = queries[0], key_rows[0], values[0]
    row_count, head_width = own_keys.shape
    cont_count = cont_queries.shape[0]
    padded = -(-cont_count // 8) * 8

    def swap(x, step):
        return lax.ppermute(x, "wide", [(i, i ^ step) for i in range(wide_count)])

    def swap_lane(x):
        return lax.ppermute(x, "narrow", [(0, 1), (1, 0)])

    message = call_kernel(
        pack_kernel,
        (lengths, log_gate, own_keys, payload_lines),
        [jax.ShapeDtypeStruct((row_count + extra_rows, 2 * head_width), jnp.bfloat16)],
        1 << 22,
    )
    far_first = swap(message, half)
    own = [message] + [None] * (half - 1)
    far = [far_first] + [None] * (half - 1)
    for step in range(half - 1, 0, -1):
        own[step] = swap(message, step)
    for step in range(half - 1, 0, -1):
        far[step] = swap(far_first, step)
    rows = jnp.pad(cont_queries, ((0, padded - cont_count), (0, 0)))
    mine = jnp.pad(cont_prompt == lane, (0, padded - cont_count))[:, None]
    sent = swap_lane(jnp.where(mine, jnp.zeros_like(rows), rows))
    cont_rows = jnp.concatenate([jnp.where(mine, rows, jnp.zeros_like(rows)), sent], axis=0)
    half_total, reach_near = call_kernel(
        near_kernel,
        (lengths, log_gate, query_rows, own_keys, payload_lines, cont_rows, *own),
        [
            jax.ShapeDtypeStruct((row_count, head_width), jnp.float32),
            jax.ShapeDtypeStruct((2 * padded, head_width), jnp.float32),
        ],
        1 << 30,
    )
    reach = call_kernel(
        reach_kernel,
        (cont_rows, reach_near, *own, *far),
        [jax.ShapeDtypeStruct((2 * padded, head_width), jnp.float32)],
        1 << 28,
    )
    returned = swap_lane(reach[padded:])
    prompt_out = call_kernel(
        far_kernel,
        (lengths, log_gate, query_rows, half_total, *own, *far),
        [jax.ShapeDtypeStruct((row_count, head_width), jnp.bfloat16)],
        1 << 30,
    )
    cont_out = rms_rows((reach[:padded] + returned)[:cont_count]).astype(jnp.bfloat16)
    return (prompt_out[None], cont_out)


def solution(mesh):
    in_specs = (
        P(("groups", "narrow"), "wide", None),
        P(("groups", "narrow"), "wide", None),
        P(("groups", "narrow"), "wide", None),
        P(("groups", "narrow"), "wide"),
        P(("groups", "narrow")),
        P(("groups", "wide", "narrow"), None),
        P(("groups", "wide", "narrow")),
    )
    out_specs = (P(("groups", "narrow"), "wide", None), P(("groups", "wide", "narrow"), None))
    gathers = mesh.shape["wide"] == 8 and mesh.shape["narrow"] == 2
    body = gathered_device if gathers else on_device
    return jax.shard_map(
        body, mesh=mesh, in_specs=in_specs, out_specs=out_specs, check_vma=False
    )
```
